32 devices in a mesh: task: 4 (over z), dp: 8 (over y, x, core).
Axes of the slice: x: 2, y: 2, z: 4, core: 2. Of those that a mesh axis runs over, the one named last changes fastest.
Arguments:
- tokens_in: bfloat16 [32768, 4096], P(('task', 'dp')), may hold values from -45 to 45
- query_cotangent: bfloat16 [32768, 2048], P(('task', 'dp')), may hold values from -5760 to 5760
- task_index: int32 [32768], P(('task', 'dp')), may hold values from 0 to 15, as said below
- loss_weights: int32 [16], replicated, may hold values from 1 to 4
- master: float32 [4096, 2048], P(('task', 'dp')), may hold values from -6 to 6
- moment_first: float32 [4096, 2048], P(('task', 'dp')), may hold values from -6 to 6
- moment_second: float32 [4096, 2048], P(('task', 'dp')), may hold values from 0.05 to 5
Outputs:
- new_master: float32 [4096, 2048], P(('task', 'dp'))
- new_first: float32 [4096, 2048], P(('task', 'dp'))
- new_second: float32 [4096, 2048], P(('task', 'dp'))
The draws below stay inside these ranges and needn't reach their ends.
Inputs may be any that keep to these rules, and one draw needn't show every extreme that they name: `task_index`: the first 16 tokens name each task once.
All inputs are finite; a program needn't handle non-finite values.
Results may differ from the reference program's by a relative error of at most 0.00042.
Values may be sent and summed in bfloat16 or wider, within the bound.
A program may use at most 192 MiB of HBM per device.

```python
import math
import jax
import jax.numpy as jnp
from jax import lax

D = 4096
QW = 2048
TASKS = 16
TOK_DEV = 1024
TOKENS = 32768
DEVICES = 32


def column_profile(key, col_count, spread):
    position = jnp.arange(col_count, dtype=jnp.float32) / col_count
    exponent = jax.random.uniform(key, (col_count,), jnp.float32)
    return 3.0 ** position * spread ** exponent


def field_values(key, row_count, col_count):
    subkeys = jax.random.split(key, 2)
    scales = column_profile(subkeys[0], col_count, 10.0)
    values = jnp.clip(jax.random.normal(subkeys[1], (row_count, col_count), jnp.float32), -6.0, 6.0)
    return values * scales[None, :] * 0.25


def draw_tokens_in(key, part):
    return field_values(jax.random.fold_in(key, 11), TOKENS, D).astype(jnp.bfloat16)


def draw_query_cotangent(key, part):
    amplitude = float(TOKENS // (TASKS * TASKS))
    inputs = field_values(jax.random.fold_in(key, 11), TOKENS, D)
    own_part = field_values(jax.random.fold_in(key, 23), TOKENS, QW)
    block_size = math.gcd(QW, 128)
    block_count = QW // block_size
    mixing = jax.random.normal(jax.random.fold_in(key, 29), (block_count, block_size, block_size), jnp.float32)
    mixing = mixing / math.sqrt(block_size)
    leading = inputs[:, :QW].reshape(TOKENS, block_count, block_size)
    carried = jnp.einsum('nbk,bkj->nbj', leading, mixing, precision=lax.Precision.HIGHEST)
    combined = jnp.clip(own_part + 0.15 * carried.reshape(TOKENS, QW), -45.0, 45.0)
    return (combined * amplitude).astype(jnp.bfloat16)


def draw_task_index(key, part):
    subkeys = jax.random.split(jax.random.fold_in(key, 37), 2)
    rows_all = jnp.arange(TOKENS, dtype=jnp.int32)
    shifted = rows_all * TASKS // TOKENS
    offsets = jax.random.randint(subkeys[0], (TOKENS,), 0, TASKS // 2, dtype=jnp.int32)
    sliding = (shifted + offsets) % TASKS
    ordering = jax.random.permutation(subkeys[1], jnp.arange(TASKS, dtype=jnp.int32))
    leading = ordering[jnp.minimum(rows_all, TASKS - 1)]
    return jnp.where(rows_all < TASKS, leading, sliding).astype(jnp.int32)


def set_ends(result, key, least, high):
    index_at = [jax.random.randint(jax.random.fold_in(key, axis), (), 0, length) for axis, length in enumerate(result.shape)]
    main_axis = result.shape.index(max(result.shape))
    neighbour = index_at[:main_axis] + [(index_at[main_axis] + 1) % result.shape[main_axis]] + index_at[main_axis + 1:]
    return result.at[tuple(index_at)].set(least).at[tuple(neighbour)].set(high)


def level_of(key, dims, shards, low, high):
    loudness = 1.0
    for dim, shards_of in shards:
        draws = jax.random.uniform(jax.random.fold_in(jax.random.fold_in(key, 6), dim), (shards_of,), jnp.float32, low / len(shards), high / len(shards))
        loudness = loudness * jnp.repeat(jnp.exp(draws), dims[dim] // shards_of).reshape((-1,) + (1,) * (len(dims) - 1 - dim))
    return loudness


def normal_values(stream_key, extent, width, limit, pieces=(), held_as=jnp.bfloat16):
    level = level_of(stream_key, extent, pieces, -0.22, 0.18) if pieces else 1.0
    array = jax.random.normal(stream_key, extent, jnp.float32) * width * level
    return jnp.minimum(jnp.maximum(array, -limit), limit).astype(held_as)


def setup_inputs(seed: int = 0) -> dict:
    key_of = jax.random.split(jax.random.key(seed), 8)
    tokens_in = draw_tokens_in(jax.random.fold_in(key_of[7], 71), 0)
    query_cotangent = draw_query_cotangent(jax.random.fold_in(key_of[7], 71), 0)
    task_index = draw_task_index(jax.random.fold_in(key_of[7], 71), 0)
    loss_weights = set_ends(jax.random.randint(key_of[3], (TASKS,), 1, 5), jax.random.fold_in(key_of[3], 1), 1, 4).astype(jnp.int32)
    master = normal_values(key_of[4], (D, QW), 1.0, 6.0, ((0, 32),), jnp.float32)
    moment_first = normal_values(key_of[5], (D, QW), 1.0, 6.0, ((0, 32),), jnp.float32)
    moment_second = jnp.clip(jnp.exp(math.log(5.0) - 4.6051702 * jax.random.uniform(key_of[6], (D, QW), jnp.float32) ** level_of(key_of[6], (D, QW), ((0, 32),), -0.2, 0.2)), 0.05, 5.0)
    return dict(tokens_in=tokens_in, query_cotangent=query_cotangent, task_index=task_index, loss_weights=loss_weights, master=master, moment_first=moment_first, moment_second=moment_second)


beta_one = 0.9
beta_two = 0.95
adam_eps = 1e-08
step_rate = 0.01
decay_rate = 0.1
corr_one = 1.0 - 0.9 ** 10
corr_two = 1.0 - 0.95 ** 10

def reference(tokens_in, query_cotangent, task_index, loss_weights, master, moment_first, moment_second):
    labels = jnp.arange(TASKS, dtype=jnp.int32)
    member = task_index[:, None] == labels[None, :]
    counts = lax.optimization_barrier(jnp.sum(member.astype(jnp.int32), axis=0))
    task_scale = loss_weights.astype(jnp.float32) / counts.astype(jnp.float32)
    token_scale = lax.optimization_barrier(jnp.sum(jnp.where(member, task_scale[None, :], jnp.float32(0.0)), axis=1))
    weighted = (query_cotangent.astype(jnp.float32) * token_scale[:, None]).astype(jnp.bfloat16)
    token_blocks = tokens_in.reshape(DEVICES, TOK_DEV, D)
    weight_blocks = weighted.reshape(DEVICES, TOK_DEV, QW)

    def add_block(running, blocks_pair):
        product = jnp.dot(blocks_pair[0].T, blocks_pair[1], preferred_element_type=jnp.float32)
        return (running + product, None)
    gradient, unused = lax.scan(add_block, jnp.zeros((D, QW), jnp.float32), (token_blocks, weight_blocks))
    square_sum = jnp.sum(gradient * gradient)
    root_mean = jnp.sqrt(square_sum / (D * QW))
    clip = 1.0 / jnp.maximum(root_mean, 1.0)
    clipped = gradient * clip
    new_first = beta_one * moment_first + (1.0 - beta_one) * clipped
    new_second = beta_two * moment_second + (1.0 - beta_two) * clipped * clipped
    direction = new_first / corr_one / (jnp.sqrt(new_second / corr_two) + adam_eps)
    new_master = master - step_rate * (direction + decay_rate * master)
    return (new_master, new_first, new_second)
```

```python
import functools

import jax
import jax.numpy as jnp
from jax import lax
from jax.experimental import pallas as pl
from jax.experimental.pallas import tpu as pltpu
from jax.sharding import PartitionSpec as P

beta_one = 0.9
beta_two = 0.95
adam_eps = 1e-08
step_rate = 0.01
decay_rate = 0.1
corr_one = 1.0 - 0.9**10
corr_two = 1.0 - 0.95**10

down = 2.0**-10
up = 2.0**10
half_type = jnp.float16
COLUMN_TILE = 512


def product_kernel(send_order, keep_order, block, index_ref, *refs):
    own = jnp.concatenate([ref[...] for ref in refs[:-5]], axis=1)
    other_ref, weight_own, weight_other, send_ref, keep_ref = refs[-5:]
    dims = (((0,), (0,)), ((), ()))
    total = lax.dot_general(own, weight_own[...], dims, preferred_element_type=jnp.float32)
    total += lax.dot_general(
        other_ref[...], weight_other[...], dims, preferred_element_type=jnp.float32
    )
    for order, out in ((send_order, send_ref), (keep_order, keep_ref)):
        for place, rank in enumerate(order):
            rows = total[rank * block : (rank + 1) * block]
            out[place * block : (place + 1) * block, :] = rows.astype(out.dtype)


def exchange_kernel(groups, lanes, in_ref, out_ref, slots, send_sems, recv_sems):
    group, lane = lax.axis_index("task"), lax.axis_index("dp")
    offsets = range(1, groups * lanes)

    def peer(offset):
        return (group ^ (offset // lanes), lane ^ (offset % lanes))

    barrier = pltpu.get_barrier_semaphore()
    for offset in offsets:
        pl.semaphore_signal(
            barrier, inc=1, device_id=peer(offset), device_id_type=pl.DeviceIdType.MESH
        )
    pl.semaphore_wait(barrier, len(offsets))
    copies = []
    for offset in offsets:
        copy = pltpu.make_async_remote_copy(
            src_ref=in_ref,
            dst_ref=slots.at[offset],
            send_sem=send_sems.at[offset],
            recv_sem=recv_sems.at[offset],
            device_id=peer(offset),
            device_id_type=pl.DeviceIdType.MESH,
        )
        copy.start()
        copies.append(copy)
    total = in_ref[...]
    for offset, copy in zip(offsets, copies):
        copy.wait_recv()
        total = total + slots[offset]
    for copy in copies:
        copy.wait_send()
    out_ref[...] = total


def sum_everywhere(value, collective_id):
    groups, lanes = lax.axis_size("task"), lax.axis_size("dp")
    devices = groups * lanes
    padded = jnp.zeros((8, 128), value.dtype).at[0, : value.size].set(value.reshape(-1))
    total = pl.pallas_call(
        functools.partial(exchange_kernel, groups, lanes),
        out_shape=jax.ShapeDtypeStruct(padded.shape, padded.dtype),
        in_specs=[pl.BlockSpec(memory_space=pltpu.VMEM)],
        out_specs=pl.BlockSpec(memory_space=pltpu.VMEM),
        scratch_shapes=[
            pltpu.VMEM((devices,) + padded.shape, padded.dtype),
            pltpu.SemaphoreType.DMA((devices,)),
            pltpu.SemaphoreType.DMA((devices,)),
        ],
        cost_estimate=pl.CostEstimate(flops=10**6, bytes_accessed=10**7, transcendentals=0),
        compiler_params=pltpu.CompilerParams(collective_id=collective_id, has_side_effects=True),
    )(padded)
    return total[0, : value.size]


def copy_kernel(index_ref, source_ref, out_ref):
    out_ref[...] = source_ref[...]


def gather_columns(indices, tokens, start, count, block):
    depth = tokens.shape[0]
    if block % 128:
        blocks = tokens.reshape(depth, tokens.shape[1] // block, block)
        taken = jnp.take(blocks, indices[start : start + count], axis=1)
        return taken.reshape(depth, count * block)
    return pl.pallas_call(
        copy_kernel,
        grid_spec=pltpu.PrefetchScalarGridSpec(
            num_scalar_prefetch=1,
            grid=(count,),
            in_specs=[pl.BlockSpec((depth, block), lambda n, s: (0, s[start + n]))],
            out_specs=pl.BlockSpec((depth, block), lambda n, s: (0, n)),
        ),
        out_shape=jax.ShapeDtypeStruct((depth, count * block), tokens.dtype),
        cost_estimate=pl.CostEstimate(
            flops=0, bytes_accessed=4 * depth * count * block, transcendentals=0
        ),
    )(indices, tokens)


def product(
    indices, start, tokens, other, weight_own, weight_other, first, width, send_order, keep_order, block
):
    depth = tokens.shape[0]
    count = len(send_order) + len(keep_order)
    tile = min(COLUMN_TILE, width)
    offset = first // tile
    own_specs = [
        pl.BlockSpec((depth, block), functools.partial(lambda r, n, s: (0, s[r]), start + r))
        for r in range(count)
    ]
    own_arrays = [tokens] * count
    if block % 128:
        own_specs = [pl.BlockSpec((depth, count * block), lambda n, s: (0, 0))]
        own_arrays = [gather_columns(indices, tokens, start, count, block)]
    weight_spec = pl.BlockSpec((depth, tile), lambda n, s: (0, offset + n))
    return pl.pallas_call(
        functools.partial(product_kernel, send_order, keep_order, block),
        grid_spec=pltpu.PrefetchScalarGridSpec(
            num_scalar_prefetch=1,
            grid=(width // tile,),
            in_specs=own_specs
            + [pl.BlockSpec((depth, count * block), lambda n, s: (0, 0)), weight_spec, weight_spec],
            out_specs=[
                pl.BlockSpec((len(send_order) * block, tile), lambda n, s: (0, n)),
                pl.BlockSpec((len(keep_order) * block, tile), lambda n, s: (0, n)),
            ],
        ),
        out_shape=[
            jax.ShapeDtypeStruct((len(send_order) * block, width), jnp.float32),
            jax.ShapeDtypeStruct((len(keep_order) * block, width), jnp.float32),
        ],
        cost_estimate=pl.CostEstimate(
            flops=4 * depth * count * block * width,
            bytes_accessed=4 * depth * (count * block + width) + 4 * count * block * width,
            transcendentals=0,
        ),
        compiler_params=pltpu.CompilerParams(vmem_limit_bytes=40 * 1024 * 1024),
    )(indices, *own_arrays, other, weight_own, weight_other)


def shards(
    tokens_in, query_cotangent, task_index, loss_weights, master, moment_first, moment_second
):
    groups = lax.axis_size("task")
    lanes = lax.axis_size("dp")
    chips = lanes // 2
    bits = chips.bit_length() - 1
    block = master.shape[0]
    features = query_cotangent.shape[1]
    entries = groups * lanes * block * features
    group = lax.axis_index("task")
    lane = lax.axis_index("dp")
    core = lane & 1
    chip = lane >> 1

    def flip_lane(value, mask):
        return lax.ppermute(value, "dp", [(i, i ^ mask) for i in range(lanes)])

    def flip_group(value, mask):
        return lax.ppermute(value, "task", [(i, i ^ mask) for i in range(groups)])

    steps = list(range(groups - 1, -1, -1))
    step_grid = lax.broadcasted_iota(jnp.int32, (2 * groups, chips), 0)
    rank_grid = lax.broadcasted_iota(jnp.int32, (2 * groups, chips), 1)
    core_grid = core ^ (step_grid & 1)
    owners = ((group ^ (step_grid >> 1)) * chips + (chip ^ rank_grid)) * 2 + core_grid
    owners = owners.reshape(2 * groups * chips)
    other_index = flip_lane(task_index, 1)
    other_cotangent = flip_lane(query_cotangent, 1)
    others = {}
    for step in steps:
        packed = gather_columns(owners, tokens_in, (2 * step + 1) * chips, chips, block)
        others[step] = flip_lane(packed, 1)

    labels = lax.iota(jnp.int32, loss_weights.shape[0])
    member = task_index[:, None] == labels[None, :]
    local_counts = jnp.sum(member.astype(jnp.int32), axis=0)
    counts = sum_everywhere(local_counts, 0)
    task_scale = loss_weights.astype(jnp.float32) / counts.astype(jnp.float32)

    def weigh(cotangent, index):
        hit = index[:, None] == labels[None, :]
        token_scale = jnp.sum(jnp.where(hit, task_scale[None, :], jnp.float32(0.0)), axis=1)
        return (cotangent.astype(jnp.float32) * (token_scale * down)[:, None]).astype(jnp.bfloat16)

    weight_own = weigh(query_cotangent, task_index)
    weight_other = weigh(other_cotangent, other_index)

    halves = [list(range(bits)), list(range(bits))[::-1]]
    width = features // len(halves)
    partials = {}
    token = owners
    for step in steps:
        for half, bit_order in enumerate(halves):
            ranks = list(range(chips))
            bit = bit_order[0] if bits else 0
            send_order = [r for r in ranks if r >> bit & 1]
            keep_order = [r for r in ranks if not r >> bit & 1]
            sent, kept = product(
                token, 2 * step * chips, tokens_in, others[step], weight_own, weight_other,
                half * width, width, send_order, keep_order, block,
            )
            sent = sent.astype(half_type)
            token, sent = lax.optimization_barrier((owners, sent))
            partials[step, half] = (keep_order, kept, flip_lane(sent, 2 << bit))

    order = sorted(
        (place + stage, -stage, step, half, stage)
        for place, step in enumerate(steps)
        for stage in range(1, bits + 1)
        for half in range(len(halves))
    )
    arrived = {}
    for _, _, step, half, stage in order:
        ranks, kept, received = partials[step, half]
        token, received = lax.optimization_barrier((token, received))
        value = kept + received.astype(jnp.float32)
        if stage < bits:
            bit = halves[half][stage]
            send_order = [r for r in ranks if r >> bit & 1]
            keep_order = [r for r in ranks if not r >> bit & 1]
            parts = {r: value[i * block : (i + 1) * block] for i, r in enumerate(ranks)}
            sent = jnp.concatenate([parts[r] for r in send_order]).astype(half_type)
            token, sent = lax.optimization_barrier((token, sent))
            kept = jnp.concatenate([parts[r] for r in keep_order])
            partials[step, half] = (keep_order, kept, flip_lane(sent, 2 << bit))
            continue
        for other in arrived.pop((step, half), []):
            value = value + other.astype(jnp.float32)
        if step:
            low = step & -step
            sent = value.astype(half_type)
            token, sent = lax.optimization_barrier((token, sent))
            arrived.setdefault((step ^ low, half), []).append(flip_group(sent, low))
        else:
            partials[step, half] = value
    sums = [partials[0, half] for half in range(len(halves))]

    gradient = jnp.concatenate(sums, axis=1) * up
    local_square = jnp.sum(gradient * gradient)
    square_sum = sum_everywhere(local_square[None], 1)[0]
    root_mean = jnp.sqrt(square_sum / entries)
    factor = 1.0 / jnp.maximum(root_mean, 1.0)
    clipped = gradient * factor
    new_first = beta_one * moment_first + (1.0 - beta_one) * clipped
    new_second = beta_two * moment_second + (1.0 - beta_two) * clipped * clipped
    direction = new_first / corr_one / (jnp.sqrt(new_second / corr_two) + adam_eps)
    new_master = master - step_rate * (direction + decay_rate * master)
    return (new_master, new_first, new_second)


def solution(mesh):
    return jax.shard_map(
        shards,
        mesh=mesh,
        in_specs=(
            P(("task", "dp"), None),
            P(("task", "dp"), None),
            P(("task", "dp")),
            P(),
            P(("task", "dp"), None),
            P(("task", "dp"), None),
            P(("task", "dp"), None),
        ),
        out_specs=(P(("task", "dp"), None), P(("task", "dp"), None), P(("task", "dp"), None)),
        check_vma=False,
    )
```
